32 devices in a mesh: head: 4 (over y, core), seq: 8 (over z, x).
Axes of the slice: x: 2, y: 2, z: 4, core: 2. Of those that a mesh axis runs over, the one named last changes fastest.
Arguments:
- queries: bfloat16 [8192, 4096], P('seq', 'head'), may hold values from -6 to 6
- keys: bfloat16 [8192, 512], P('seq', 'head'), may hold values from -6 to 6
- values: bfloat16 [8192, 512], P('seq', 'head'), may hold values from -6 to 6
- vertical: int32 [32, 8], P('head'), may hold values from 0 to 63, as said below
- slash: int32 [32, 8], P('head'), may hold values from 1 to 28, as said below
Outputs:
- attended: bfloat16 [8192, 4096], P(('seq', 'head'))
The draws below stay inside these ranges and needn't reach their ends.
Inputs may be any that keep to these rules, and one draw needn't show every extreme that they name: `vertical`: each row names 8 different blocks. Within each group of 8 consecutive rows, the different blocks named that lie in one slab (blocks s * 8 to s * 8 + 7) number at most 4, and exactly 4 in some slab. `slash`: each row names 8 different offsets.
All inputs are finite; a program needn't handle non-finite values.
Results may differ from the reference program's by a relative error of at most 0.0033.
Values may be sent and summed in bfloat16 or wider, within the bound.
A program may use at most 128 MiB of HBM per device.

```python
import math
import jax
import jax.numpy as jnp
from jax import lax

HD = 128
QUERY_PER_GROUP = 8
BLK = 128
VERTICAL_BLOCKS = 8
SLASH_OFFSETS = 8
LARGEST_OFFSET = 28
CAP = 4
GROUPS = 4
HEADS = 32
BLK_DEV = 8
SLABS = 8
SEQ = 8192
BLOCKS = 64


def draw_queries(key, part):
    own_key = jax.random.fold_in(key, 11)
    drawn = jnp.clip(1.5 * jax.random.normal(own_key, (SEQ, GROUPS, QUERY_PER_GROUP, HD), jnp.float32), -6.0, 6.0)
    return drawn.reshape(SEQ, HEADS * HD).astype(jnp.bfloat16)


def draw_keys(key, part):
    own_key = jax.random.fold_in(key, 12)
    drawn = jnp.clip(1.5 * jax.random.normal(own_key, (SEQ, GROUPS, HD), jnp.float32), -6.0, 6.0)
    return drawn.reshape(SEQ, GROUPS * HD).astype(jnp.bfloat16)


def vertical_group(key):
    key_count, key_full, key_order, key_pick = jax.random.split(key, 4)
    slab_ids = jnp.arange(SLABS, dtype=jnp.int32)
    counts = jax.random.randint(key_count, (SLABS,), 1, CAP + 1)
    fullest = jax.random.randint(key_full, (), 0, SLABS)
    counts = jnp.where(slab_ids == fullest, CAP, counts)
    order_scores = jax.random.randint(key_order, (SLABS, BLK_DEV), 0, 4096) * BLK_DEV + jnp.arange(BLK_DEV, dtype=jnp.int32)[None, :]
    ranks = jnp.argsort(jnp.argsort(order_scores, axis=1), axis=1)
    inside = ranks < counts[:, None]
    mandatory_blocks = (inside & (slab_ids[:, None] == fullest)).reshape(BLOCKS)
    inside = inside.reshape(BLOCKS)
    selected_indices = jax.random.randint(key_pick, (QUERY_PER_GROUP, BLOCKS), 0, 65536) * BLOCKS + jnp.arange(BLOCKS, dtype=jnp.int32)[None, :] + 1
    selected_indices = jnp.where(inside[None, :], selected_indices, 0)
    extra_score = jnp.where((jnp.arange(QUERY_PER_GROUP)[:, None] == 0) & mandatory_blocks[None, :], 1 << 29, 0)
    leftover_slots, selected_blocks = lax.top_k(selected_indices + extra_score, VERTICAL_BLOCKS)
    return selected_blocks.astype(jnp.int32)


def draw_vertical(key, part):
    group_keys = jax.random.split(jax.random.fold_in(key, 31), GROUPS)
    return jax.vmap(vertical_group)(group_keys).reshape(HEADS, VERTICAL_BLOCKS).astype(jnp.int32)


def draw_slash(key, part):
    block_scores = jax.random.randint(jax.random.fold_in(key, 41), (HEADS, LARGEST_OFFSET), 0, 65536) * LARGEST_OFFSET + jnp.arange(LARGEST_OFFSET, dtype=jnp.int32)[None, :] + 1
    per_head_rows = jnp.arange(HEADS)[:, None]
    offset_columns = jnp.arange(LARGEST_OFFSET)[None, :]
    extra_score = jnp.where((per_head_rows == 0) & (offset_columns == LARGEST_OFFSET - 1), 1 << 28, 0)
    extra_score = extra_score + jnp.where((per_head_rows == 1) & (offset_columns == 0), 1 << 28, 0)
    leftover_slots, selected_blocks = lax.top_k(block_scores + extra_score, SLASH_OFFSETS)
    return (selected_blocks + 1).astype(jnp.int32)


def block_levels(key, extent, pieces, least, largest):
    factor_of, own = 1.0, jax.random.fold_in(key, 6)
    for position, shards_of in pieces:
        steps = jnp.exp(jax.random.uniform(jax.random.fold_in(own, position), (shards_of,), jnp.float32, least / len(pieces), largest / len(pieces)))
        factor_of = factor_of * jnp.repeat(steps, extent[position] // shards_of).reshape([-1 if axis == position else 1 for axis in range(len(extent))])
    return factor_of


def normal_values(rng, dims, scale, limit, cuts=(), held_as=jnp.bfloat16):
    level = block_levels(rng, dims, cuts, -0.22, 0.18) if cuts else 1.0
    values = jax.random.normal(rng, dims, jnp.float32) * scale * level
    return jnp.minimum(jnp.maximum(values, -limit), limit).astype(held_as)


def setup_inputs(seed: int = 0) -> dict:
    key_list = jax.random.split(jax.random.key(seed), 6)
    return {
        "queries": draw_queries(jax.random.fold_in(key_list[5], 71), 0),
        "keys": draw_keys(jax.random.fold_in(key_list[5], 71), 0),
        "values": normal_values(key_list[2], (SEQ, GROUPS * HD), 1.0, 6.0, ((0, 8), (1, 4))),
        "vertical": draw_vertical(jax.random.fold_in(key_list[5], 71), 0),
        "slash": draw_slash(jax.random.fold_in(key_list[5], 71), 0),
    }


NEG = -1e+30

def attend(query_block, diag_kv, slash_kv, column_kv, slash_ok, column_ok):
    block_count, block_width, head_width = query_block.shape
    slash_count = slash_kv.shape[1]
    column_count = column_kv.shape[0]
    score_scale = 1.0 / math.sqrt(head_width)
    causal = jnp.arange(block_width)[:, None] >= jnp.arange(block_width)[None, :]
    diag_scores = jnp.einsum('ird,icd->irc', query_block, diag_kv[..., :head_width]) * score_scale
    diag_scores = jnp.where(causal[None], diag_scores, NEG)
    slash_scores = jnp.einsum('ird,ijcd->irjc', query_block, slash_kv[..., :head_width]) * score_scale
    slash_scores = jnp.where(slash_ok[:, None, :, None], slash_scores, NEG).reshape(block_count, block_width, slash_count * block_width)
    column_scores = jnp.einsum('ird,jcd->irjc', query_block, column_kv[..., :head_width]) * score_scale
    column_scores = jnp.where(column_ok[:, None, :, None], column_scores, NEG).reshape(block_count, block_width, column_count * block_width)
    block_scores = jnp.concatenate([diag_scores, slash_scores, column_scores], axis=2)
    row_top = lax.optimization_barrier(jnp.max(block_scores, axis=2, keepdims=True))
    weights = jnp.exp(block_scores - row_top)
    row_total = lax.optimization_barrier(jnp.sum(weights, axis=2))
    rounded = lax.optimization_barrier(weights.astype(jnp.bfloat16)).astype(jnp.float32)
    split_one = block_width
    split_two = block_width + slash_count * block_width
    w_diag = rounded[:, :, :split_one]
    w_slash = rounded[:, :, split_one:split_two].reshape(block_count, block_width, slash_count, block_width)
    w_column = rounded[:, :, split_two:].reshape(block_count, block_width, column_count, block_width)
    mixed_sum = jnp.einsum('irc,icd->ird', w_diag, diag_kv[..., head_width:])
    mixed_sum = mixed_sum + jnp.einsum('irjc,ijcd->ird', w_slash, slash_kv[..., head_width:])
    mixed_sum = mixed_sum + jnp.einsum('irjc,jcd->ird', w_column, column_kv[..., head_width:])
    return (mixed_sum / row_total[:, :, None]).astype(jnp.bfloat16)

def reference(queries, keys, values, vertical, slash):
    seq_rows = queries.shape[0]
    block_total = seq_rows // BLK
    joined = jnp.concatenate([keys.reshape(seq_rows, GROUPS, HD), values.reshape(seq_rows, GROUPS, HD)], axis=2)
    block_ids = jnp.arange(block_total, dtype=jnp.int32)

    def one_head(head_index):
        group_index = head_index // QUERY_PER_GROUP
        query_block = lax.dynamic_slice_in_dim(queries, head_index * HD, HD, 1).astype(jnp.float32).reshape(block_total, BLK, HD)
        group_kv = lax.dynamic_index_in_dim(joined, group_index, 1, keepdims=False).astype(jnp.float32).reshape(block_total, BLK, 2 * HD)
        padded = jnp.concatenate([jnp.zeros((LARGEST_OFFSET, BLK, 2 * HD), jnp.float32), group_kv], axis=0)
        offsets = lax.dynamic_index_in_dim(slash, head_index, 0, keepdims=False)
        columns = lax.dynamic_index_in_dim(vertical, head_index, 0, keepdims=False)
        slash_index = (LARGEST_OFFSET + block_ids[:, None] - offsets[None, :]).astype(jnp.int32)
        slash_kv = jnp.take(padded, slash_index, axis=0)
        slash_ok = block_ids[:, None] - offsets[None, :] >= 0
        column_kv = jnp.take(group_kv, columns.astype(jnp.int32), axis=0)
        covered = jnp.any(block_ids[:, None, None] - columns[None, :, None] == offsets[None, None, :], axis=2)
        column_ok = (columns[None, :] < block_ids[:, None]) & jnp.logical_not(covered)
        return attend(query_block, group_kv, slash_kv, column_kv, slash_ok, column_ok)
    outputs = lax.map(one_head, jnp.arange(HEADS, dtype=jnp.int32))
    return jnp.transpose(outputs, (1, 2, 0, 3)).reshape(seq_rows, HEADS * HD)
```

```python
import functools
import math

import jax
import jax.numpy as jnp
from jax import lax
from jax.experimental import pallas as pl
from jax.experimental.pallas import tpu as pltpu
from jax.sharding import PartitionSpec as P

BLK = 128
NEG = -1e30


def attention_kernel(slab_ref, index_ref, bias_ref, q_ref, kt_ref, v_ref, out_ref, *, blocks, listed, width):
    head = pl.program_id(0)
    base = slab_ref[0] * blocks
    factor = math.log2(math.e) / math.sqrt(width)
    causal = lax.broadcasted_iota(jnp.int32, (BLK, BLK), 0) >= lax.broadcasted_iota(
        jnp.int32, (BLK, BLK), 1
    )

    def one_block(i, carry):
        rows = pl.ds(pl.multiple_of(i * BLK, BLK), BLK)
        q = q_ref[rows, :]
        row = (head * blocks + i) * listed
        own = base + i
        scores = [
            jnp.where(causal, jnp.dot(q, kt_ref[own], preferred_element_type=jnp.float32), NEG)
        ]
        for n in range(0, listed, 2):
            a, b = index_ref[row + n], index_ref[row + n + 1]
            pair = jnp.dot(
                q, jnp.concatenate([kt_ref[a], kt_ref[b]], axis=1), preferred_element_type=jnp.float32
            )
            scores.append(pair[:, :BLK] + bias_ref[row + n])
            scores.append(pair[:, BLK:] + bias_ref[row + n + 1])
        top = functools.reduce(jnp.maximum, scores)
        top = jnp.max(top, axis=1, keepdims=True) * factor
        total = None
        rounded = []
        for s in scores:
            w = jnp.exp2(s * factor - top)
            total = w if total is None else total + w
            rounded.append(w.astype(jnp.bfloat16))
        mixed = jnp.dot(rounded[0], v_ref[own], preferred_element_type=jnp.float32)
        for n in range(0, listed, 2):
            a, b = index_ref[row + n], index_ref[row + n + 1]
            mixed += jnp.dot(
                jnp.concatenate([rounded[1 + n], rounded[2 + n]], axis=1),
                jnp.concatenate([v_ref[a], v_ref[b]], axis=0),
                preferred_element_type=jnp.float32,
            )
        total = jnp.sum(total, axis=1, keepdims=True)
        out_ref[rows, :] = (mixed / total).astype(jnp.bfloat16)
        return carry

    lax.fori_loop(0, blocks, one_block, 0, unroll=2)


def block_lists(vertical, slash, slab_index, blocks):
    ids = slab_index * blocks + jnp.arange(blocks, dtype=jnp.int32)
    slash_ids = ids[None, :, None] - slash[:, None, :]
    slash_ok = slash_ids >= 0
    columns = jnp.broadcast_to(vertical[:, None, :], slash_ids.shape[:2] + vertical.shape[1:])
    covered = jnp.any(columns[..., None] == slash_ids[:, :, None, :], axis=3)
    column_ok = (columns < ids[None, :, None]) & jnp.logical_not(covered)
    listed = jnp.concatenate([slash_ids, columns], axis=2)
    ok = jnp.concatenate([slash_ok, column_ok], axis=2)
    index = jnp.where(ok, listed, ids[None, :, None])
    bias = jnp.where(ok, 0.0, NEG).astype(jnp.float32)
    return index.reshape(-1), bias.reshape(-1), listed.shape[2]


def shards(queries, keys, values, vertical, slash):
    width = keys.shape[1]
    rows = queries.shape[0]
    blocks = rows // BLK
    heads = vertical.shape[0]
    slab_index = lax.axis_index("seq")
    kt = jnp.swapaxes(keys.reshape(blocks, BLK, width), 1, 2)
    v = values.reshape(blocks, BLK, width)
    index, bias, listed = block_lists(vertical, slash, slab_index, blocks)
    kt_all = lax.all_gather(kt, "seq", axis=0, tiled=True)
    v_all = lax.all_gather(v, "seq", axis=0, tiled=True)
    attended = pl.pallas_call(
        functools.partial(attention_kernel, blocks=blocks, listed=listed, width=width),
        grid_spec=pltpu.PrefetchScalarGridSpec(
            num_scalar_prefetch=3,
            grid=(heads,),
            in_specs=[
                pl.BlockSpec((rows, width), lambda h, *_: (0, h)),
                pl.BlockSpec(memory_space=pltpu.VMEM),
                pl.BlockSpec(memory_space=pltpu.VMEM),
            ],
            out_specs=pl.BlockSpec((rows, width), lambda h, *_: (0, h)),
        ),
        out_shape=jax.ShapeDtypeStruct((rows, heads * width), jnp.bfloat16),
        compiler_params=pltpu.CompilerParams(
            dimension_semantics=("arbitrary",), vmem_limit_bytes=60 * 1024 * 1024
        ),
    )(slab_index.reshape(1).astype(jnp.int32), index, bias, queries, kt_all, v_all)
    return lax.all_to_all(attended, "head", split_axis=0, concat_axis=1, tiled=True)


def solution(mesh):
    in_specs = (
        P("seq", "head"),
        P("seq", "head"),
        P("seq", "head"),
        P("head", None),
        P("head", None),
    )
    out_specs = P(("seq", "head"), None)
    return jax.shard_map(shards, mesh=mesh, in_specs=in_specs, out_specs=out_specs, check_vma=False)
```

```python
import functools
import math

import jax
import jax.numpy as jnp
from jax import lax
from jax.experimental import pallas as pl
from jax.experimental.pallas import tpu as pltpu
from jax.sharding import PartitionSpec as P

BLK = 128
NEG = -1e30
PIECES = 2
MESH = pl.DeviceIdType.MESH


def attend_block(q, own, row, index_ref, bias_ref, kt_ref, v_ref, causal, listed, factor):
    scores = [jnp.where(causal, jnp.dot(q, kt_ref[own], preferred_element_type=jnp.float32), NEG)]
    for n in range(0, listed, 2):
        a, b = index_ref[row + n], index_ref[row + n + 1]
        pair = jnp.dot(
            q, jnp.concatenate([kt_ref[a], kt_ref[b]], axis=1), preferred_element_type=jnp.float32
        )
        scores.append(pair[:, :BLK] + bias_ref[row + n])
        scores.append(pair[:, BLK:] + bias_ref[row + n + 1])
    top = functools.reduce(jnp.maximum, scores)
    top = jnp.max(top, axis=1, keepdims=True) * factor
    total = None
    rounded = []
    for s in scores:
        w = jnp.exp2(s * factor - top)
        total = w if total is None else total + w
        rounded.append(w.astype(jnp.bfloat16))
    mixed = jnp.dot(rounded[0], v_ref[own], preferred_element_type=jnp.float32)
    for n in range(0, listed, 2):
        a, b = index_ref[row + n], index_ref[row + n + 1]
        mixed += jnp.dot(
            jnp.concatenate([rounded[1 + n], rounded[2 + n]], axis=1),
            jnp.concatenate([v_ref[a], v_ref[b]], axis=0),
            preferred_element_type=jnp.float32,
        )
    total = jnp.sum(total, axis=1, keepdims=True)
    return (mixed / total).astype(jnp.bfloat16)


def layer_kernel(
    index_ref,
    bias_ref,
    q_ref,
    kt_ref,
    v_ref,
    out_ref,
    kt_buf,
    v_buf,
    staged,
    load_sem,
    chain_send,
    chain_recv,
    cross_send,
    cross_recv,
    out_local,
    out_send,
    out_recv,
    *,
    blocks,
    listed,
    width,
    heads,
    slabs,
    groups,
):
    slab = lax.axis_index("seq")
    group = lax.axis_index("head")
    chain_len = slabs // 2
    place, side = slab // 2, slab % 2
    piece = blocks // PIECES
    bufs = (kt_buf, v_buf)
    has_next = place + 1 < chain_len

    def part(kv, place_of, side_of, c):
        first = pl.multiple_of((place_of * 2 + side_of) * blocks + c * piece, piece)
        return bufs[kv].at[pl.ds(first, piece)]

    def chain(t, kv, c):
        ref = part(kv, place - t, side, c)
        return pltpu.make_async_remote_copy(
            ref, ref, chain_send.at[t, kv, c], chain_recv.at[t, kv, c],
            device_id={"seq": slab + 2}, device_id_type=MESH,
        )

    def chain_in(t, kv, c):
        ref = part(kv, place - t, side, c)
        return pltpu.make_async_remote_copy(
            ref, ref, chain_send.at[t - 1, kv, c], chain_recv.at[t - 1, kv, c],
            device_id={"seq": slab - 2}, device_id_type=MESH,
        )

    def cross(t, kv, c, side_of):
        ref = part(kv, place - t, side_of, c)
        return pltpu.make_async_remote_copy(
            ref, ref, cross_send.at[t, kv, c], cross_recv.at[t, kv, c],
            device_id={"seq": place * 2 + 1 - side}, device_id_type=MESH,
        )

    def sends_cross(t):
        return side == 0 if t == 0 else place >= t

    def gets_cross(t):
        return side == 1 if t == 0 else place >= t

    own_first = pl.multiple_of(slab * blocks, blocks)
    loads = [
        pltpu.make_async_copy(src, buf.at[pl.ds(own_first, blocks)], load_sem.at[kv])
        for kv, (src, buf) in enumerate(((kt_ref, kt_buf), (v_ref, v_buf)))
    ]
    for load in loads:
        load.start()

    barrier = pltpu.get_barrier_semaphore()
    pl.semaphore_signal(
        barrier, 1, device_id={"seq": place * 2 + 1 - side}, device_id_type=MESH
    )
    for d in range(1, groups):
        pl.semaphore_signal(
            barrier, 1, device_id={"head": lax.rem(group + d, groups)}, device_id_type=MESH
        )

    @pl.when(has_next)
    def _():
        pl.semaphore_signal(barrier, 1, device_id={"seq": slab + 2}, device_id_type=MESH)

    @pl.when(place > 0)
    def _():
        pl.semaphore_signal(barrier, 1, device_id={"seq": slab - 2}, device_id_type=MESH)

    pl.semaphore_wait(
        barrier, groups + has_next.astype(jnp.int32) + (place > 0).astype(jnp.int32)
    )
    for load in loads:
        load.wait()

    for kv in range(2):
        for t in range(chain_len):
            for c in range(PIECES):
                if t > 0:

                    @pl.when(place >= t)
                    def _():
                        chain_in(t, kv, c).wait_recv()

                if t < chain_len - 1:

                    @pl.when((place >= t) & has_next)
                    def _():
                        chain(t, kv, c).start()

                @pl.when(sends_cross(t))
                def _():
                    cross(t, kv, c, side).start()

    for kv in range(2):
        for t in range(chain_len):
            for c in range(PIECES):

                @pl.when(gets_cross(t))
                def _():
                    cross(t, kv, c, 1 - side).wait_recv()

    factor = math.log2(math.e) / math.sqrt(width)
    causal = lax.broadcasted_iota(jnp.int32, (BLK, BLK), 0) >= lax.broadcasted_iota(
        jnp.int32, (BLK, BLK), 1
    )
    share = blocks // groups
    share_rows = share * BLK
    base = slab * blocks

    def out_columns(group_of, head):
        return pl.ds(pl.multiple_of((group_of * heads + head) * width, width), width)

    def out_copy(head, r):
        owner = lax.rem(group + 1 + r, groups)
        return pltpu.make_async_remote_copy(
            staged.at[head, pl.ds(pl.multiple_of(owner * share_rows, share_rows), share_rows)],
            out_ref.at[:, out_columns(group, head)],
            out_send.at[head, r], out_recv.at[head, r],
            device_id={"head": owner}, device_id_type=MESH,
        )

    def out_in(head, r):
        sender = lax.rem(group + groups - 1 - r, groups)
        return pltpu.make_async_remote_copy(
            staged.at[head, pl.ds(0, share_rows)],
            out_ref.at[:, out_columns(sender, head)],
            out_send.at[head, r], out_recv.at[head, r],
            device_id={"head": sender}, device_id_type=MESH,
        )

    def out_own(head):
        return pltpu.make_async_copy(
            staged.at[head, pl.ds(pl.multiple_of(group * share_rows, share_rows), share_rows)],
            out_ref.at[:, out_columns(group, head)],
            out_local.at[head],
        )

    def one_share(step, carry):
        head, r = step // groups, step % groups
        owner = lax.rem(group + 1 + r, groups)
        columns = pl.ds(pl.multiple_of(head * width, width), width)
        for u in range(share):
            i = owner * share + u
            rows = pl.ds(pl.multiple_of(i * BLK, BLK), BLK)
            row = (head * blocks + i) * listed
            staged[head, rows, :] = attend_block(
                q_ref[rows, columns], base + i, row, index_ref, bias_ref, kt_buf, v_buf,
                causal, listed, factor,
            )

        @pl.when(r < groups - 1)
        def _():
            out_copy(head, r).start()

        @pl.when(r == groups - 1)
        def _():
            out_own(head).start()

        return carry

    lax.fori_loop(0, heads * groups, one_share, 0)

    for kv in range(2):
        for t in range(chain_len):
            for c in range(PIECES):
                if t < chain_len - 1:

                    @pl.when((place >= t) & has_next)
                    def _():
                        chain(t, kv, c).wait_send()

                @pl.when(sends_cross(t))
                def _():
                    cross(t, kv, c, side).wait_send()

    def finish(head, carry):
        out_own(head).wait()
        for r in range(groups - 1):
            out_copy(head, r).wait_send()
            out_in(head, r).wait_recv()
        return carry

    lax.fori_loop(0, heads, finish, 0)


def block_lists(vertical, slash, slab_index, blocks):
    ids = slab_index * blocks + jnp.arange(blocks, dtype=jnp.int32)
    slash_ids = ids[None, :, None] - slash[:, None, :]
    slash_ok = slash_ids >= 0
    columns = jnp.broadcast_to(vertical[:, None, :], slash_ids.shape[:2] + vertical.shape[1:])
    covered = jnp.any(columns[..., None] == slash_ids[:, :, None, :], axis=3)
    column_ok = (columns < ids[None, :, None]) & jnp.logical_not(covered)
    listed = jnp.concatenate([slash_ids, columns], axis=2)
    ok = jnp.concatenate([slash_ok, column_ok], axis=2)
    index = jnp.where(ok, listed, ids[None, :, None])
    bias = jnp.where(ok, 0.0, NEG).astype(jnp.float32)
    return index.reshape(-1), bias.reshape(-1), listed.shape[2]


def shards(queries, keys, values, vertical, slash):
    width = keys.shape[1]
    rows = queries.shape[0]
    blocks = rows // BLK
    heads = vertical.shape[0]
    slabs, groups = lax.axis_size("seq"), lax.axis_size("head")
    kt = jnp.swapaxes(keys.reshape(blocks, BLK, width), 1, 2)
    v = values.reshape(blocks, BLK, width)
    index, bias, listed = block_lists(vertical, slash, lax.axis_index("seq"), blocks)
    dma = pltpu.SemaphoreType.DMA
    hops = (slabs // 2, 2, PIECES)
    smem, anywhere = pl.BlockSpec(memory_space=pltpu.SMEM), pl.BlockSpec(memory_space=pl.ANY)
    return pl.pallas_call(
        functools.partial(
            layer_kernel,
            blocks=blocks,
            listed=listed,
            width=width,
            heads=heads,
            slabs=slabs,
            groups=groups,
        ),
        in_specs=[smem, smem, pl.BlockSpec(memory_space=pltpu.VMEM), anywhere, anywhere],
        out_specs=anywhere,
        out_shape=jax.ShapeDtypeStruct((rows // groups, groups * heads * width), jnp.bfloat16),
        scratch_shapes=[
            pltpu.VMEM((slabs * blocks, width, BLK), jnp.bfloat16),
            pltpu.VMEM((slabs * blocks, BLK, width), jnp.bfloat16),
            pltpu.VMEM((heads, rows, width), jnp.bfloat16),
            dma((2,)),
            dma(hops),
            dma(hops),
            dma(hops),
            dma(hops),
            dma((heads,)),
            dma((heads, groups - 1)),
            dma((heads, groups - 1)),
        ],
        compiler_params=pltpu.CompilerParams(
            collective_id=0, has_side_effects=True, vmem_limit_bytes=60 * 1024 * 1024
        ),
    )(index, bias, queries, kt, v)


def solution(mesh):
    in_specs = (
        P("seq", "head"),
        P("seq", "head"),
        P("seq", "head"),
        P("head", None),
        P("head", None),
    )
    out_specs = P(("seq", "head"), None)
    return jax.shard_map(shards, mesh=mesh, in_specs=in_specs, out_specs=out_specs, check_vma=False)
```

```python
import functools
import math

import jax
import jax.numpy as jnp
from jax import lax
from jax.experimental import pallas as pl
from jax.experimental.pallas import tpu as pltpu
from jax.sharding import PartitionSpec as P

BLK = 128
NEG = -1e30
PIECES = 2
EARLY = 6
VALUE_STRIDE = 3
MESH = pl.DeviceIdType.MESH


def block_weights(q, own, row, index_ref, bias_ref, kt_ref, causal, listed, factor):
    scores = [jnp.where(causal, jnp.dot(q, kt_ref[own], preferred_element_type=jnp.float32), NEG)]
    for n in range(0, listed, 2):
        a, b = index_ref[row + n], index_ref[row + n + 1]
        pair = jnp.dot(
            q, jnp.concatenate([kt_ref[a], kt_ref[b]], axis=1), preferred_element_type=jnp.float32
        )
        scores.append(pair[:, :BLK] + bias_ref[row + n])
        scores.append(pair[:, BLK:] + bias_ref[row + n + 1])
    top = functools.reduce(jnp.maximum, scores)
    top = jnp.max(top, axis=1, keepdims=True) * factor
    total = None
    rounded = []
    for s in scores:
        w = jnp.exp2(s * factor - top)
        total = w if total is None else total + w
        rounded.append(w.astype(jnp.bfloat16))
    return rounded, jnp.sum(total, axis=1, keepdims=True)


def block_mix(own_weights, pair_weights, total, own, row, index_ref, v_ref, listed):
    mixed = jnp.dot(own_weights, v_ref[own], preferred_element_type=jnp.float32)
    for n in range(0, listed, 2):
        a, b = index_ref[row + n], index_ref[row + n + 1]
        mixed += jnp.dot(
            pair_weights(n),
            jnp.concatenate([v_ref[a], v_ref[b]], axis=0),
            preferred_element_type=jnp.float32,
        )
    return (mixed / total).astype(jnp.bfloat16)


def layer_kernel(
    slash_ref,
    vertical_ref,
    queries_ref,
    kt_ref,
    v_ref,
    out_ref,
    index_ref,
    bias_ref,
    q_ref,
    kt_buf,
    v_buf,
    staged,
    early_weights,
    early_total,
    load_sem,
    chain_send,
    chain_recv,
    cross_send,
    cross_recv,
    out_local,
    out_send,
    out_recv,
    *,
    blocks,
    listed,
    width,
    heads,
    slabs,
    groups,
):
    slab = lax.axis_index("seq")
    group = lax.axis_index("head")
    chain_len = slabs // 2
    place, side = slab // 2, slab % 2
    piece = blocks // PIECES
    bufs = (kt_buf, v_buf)
    has_next = place + 1 < chain_len

    def part(kv, place_of, side_of, c):
        first = pl.multiple_of((place_of * 2 + side_of) * blocks + c * piece, piece)
        return bufs[kv].at[pl.ds(first, piece)]

    def chain(t, kv, c):
        ref = part(kv, place - t, side, c)
        return pltpu.make_async_remote_copy(
            ref, ref, chain_send.at[t, kv, c], chain_recv.at[t, kv, c],
            device_id={"seq": slab + 2}, device_id_type=MESH,
        )

    def chain_in(t, kv, c):
        ref = part(kv, place - t, side, c)
        return pltpu.make_async_remote_copy(
            ref, ref, chain_send.at[t - 1, kv, c], chain_recv.at[t - 1, kv, c],
            device_id={"seq": slab - 2}, device_id_type=MESH,
        )

    def cross(t, kv, c, side_of):
        ref = part(kv, place - t, side_of, c)
        return pltpu.make_async_remote_copy(
            ref, ref, cross_send.at[t, kv, c], cross_recv.at[t, kv, c],
            device_id={"seq": place * 2 + 1 - side}, device_id_type=MESH,
        )

    def sends_cross(t):
        return side == 0 if t == 0 else place >= t

    def gets_cross(t):
        return side == 1 if t == 0 else place >= t

    own_first = pl.multiple_of(slab * blocks, blocks)
    loads = [
        pltpu.make_async_copy(src, buf.at[pl.ds(own_first, blocks)], load_sem.at[kv])
        for kv, (src, buf) in enumerate(((kt_ref, kt_buf), (v_ref, v_buf)))
    ]
    loads.append(pltpu.make_async_copy(queries_ref, q_ref, load_sem.at[2]))
    for load in loads:
        load.start()

    barrier = pltpu.get_barrier_semaphore()
    pl.semaphore_signal(
        barrier, 1, device_id={"seq": place * 2 + 1 - side}, device_id_type=MESH
    )
    for d in range(1, groups):
        pl.semaphore_signal(
            barrier, 1, device_id={"head": lax.rem(group + d, groups)}, device_id_type=MESH
        )

    @pl.when(has_next)
    def _():
        pl.semaphore_signal(barrier, 1, device_id={"seq": slab + 2}, device_id_type=MESH)

    @pl.when(place > 0)
    def _():
        pl.semaphore_signal(barrier, 1, device_id={"seq": slab - 2}, device_id_type=MESH)

    pl.semaphore_wait(
        barrier, groups + has_next.astype(jnp.int32) + (place > 0).astype(jnp.int32)
    )
    def pass_on(t, kv, c):
        if t > 0:

            @pl.when(place >= t)
            def _():
                chain_in(t, kv, c).wait_recv()

        if t < chain_len - 1:

            @pl.when((place >= t) & has_next)
            def _():
                chain(t, kv, c).start()

        @pl.when(sends_cross(t))
        def _():
            cross(t, kv, c, side).start()

    def wait_cross(kv):
        for t in range(chain_len):
            for c in range(PIECES):

                @pl.when(gets_cross(t))
                def _():
                    cross(t, kv, c, 1 - side).wait_recv()

    base = slab * blocks
    slashes, verticals = slash_ref.shape[1], vertical_ref.shape[1]

    def list_blocks(step, carry):
        head, own = step // blocks, base + step % blocks
        reached = [own - slash_ref[head, n] for n in range(slashes)]
        for n, block in enumerate(reached):
            ok = block >= 0
            index_ref[step * listed + n] = jnp.where(ok, block, own)
            bias_ref[step * listed + n] = jnp.where(ok, 0.0, NEG)
        for n in range(verticals):
            block = vertical_ref[head, n]
            ok = block < own
            for other in reached:
                ok = ok & (block != other)
            index_ref[step * listed + slashes + n] = jnp.where(ok, block, own)
            bias_ref[step * listed + slashes + n] = jnp.where(ok, 0.0, NEG)
        return carry

    loads[0].wait()
    for c in range(PIECES):
        pass_on(0, 0, c)
    lax.fori_loop(0, heads * blocks, list_blocks, 0)
    for t in range(1, chain_len):
        for c in range(PIECES):
            pass_on(t, 0, c)
    loads[1].wait()
    for c in range(PIECES):
        pass_on(0, 1, c)
    wait_cross(0)
    loads[2].wait()

    factor = math.log2(math.e) / math.sqrt(width)
    causal = lax.broadcasted_iota(jnp.int32, (BLK, BLK), 0) >= lax.broadcasted_iota(
        jnp.int32, (BLK, BLK), 1
    )
    share = blocks // groups
    share_rows = share * BLK

    def out_columns(group_of, head):
        return pl.ds(pl.multiple_of((group_of * heads + head) * width, width), width)

    def out_copy(head, r):
        owner = lax.rem(group + 1 + r, groups)
        return pltpu.make_async_remote_copy(
            staged.at[head, pl.ds(pl.multiple_of(owner * share_rows, share_rows), share_rows)],
            out_ref.at[:, out_columns(group, head)],
            out_send.at[head, r], out_recv.at[head, r],
            device_id={"head": owner}, device_id_type=MESH,
        )

    def out_in(head, r):
        sender = lax.rem(group + groups - 1 - r, groups)
        return pltpu.make_async_remote_copy(
            staged.at[head, pl.ds(0, share_rows)],
            out_ref.at[:, out_columns(sender, head)],
            out_send.at[head, r], out_recv.at[head, r],
            device_id={"head": sender}, device_id_type=MESH,
        )

    def out_own(head):
        return pltpu.make_async_copy(
            staged.at[head, pl.ds(pl.multiple_of(group * share_rows, share_rows), share_rows)],
            out_ref.at[:, out_columns(group, head)],
            out_local.at[head],
        )

    early = early_weights.shape[0]
    values_due = [(t, c) for t in range(1, chain_len) for c in range(PIECES)]

    def owned_blocks(step):
        head, r = step // groups, step % groups
        owner = lax.rem(group + 1 + r, groups)
        columns = pl.ds(pl.multiple_of(head * width, width), width)
        for u in range(share):
            i = owner * share + u
            rows = pl.ds(pl.multiple_of(i * BLK, BLK), BLK)
            yield head, rows, columns, base + i, (head * blocks + i) * listed

    def send_share(step):
        head, r = step // groups, step % groups

        @pl.when(r < groups - 1)
        def _():
            out_copy(head, r).start()

        @pl.when(r == groups - 1)
        def _():
            out_own(head).start()

    def weigh_early(step, carry):
        for k, (t, c) in enumerate(values_due):

            @pl.when(step == min(VALUE_STRIDE * (k + 1), early * groups - 1))
            def _():
                pass_on(t, 1, c)

        for head, rows, columns, own, row in owned_blocks(step):
            rounded, total = block_weights(
                q_ref[rows, columns], own, row, index_ref, bias_ref, kt_buf, causal, listed, factor
            )
            for n, w in enumerate(rounded):
                early_weights[head, rows, n * BLK : (n + 1) * BLK] = w
            early_total[head, rows, :] = jnp.broadcast_to(total, (BLK, width))
        return carry

    def mix_early(step, carry):
        for head, rows, columns, own, row in owned_blocks(step):
            staged[head, rows, :] = block_mix(
                early_weights[head, rows, :BLK],
                lambda n: early_weights[head, rows, (n + 1) * BLK : (n + 3) * BLK],
                early_total[head, rows, :],
                own, row, index_ref, v_buf, listed,
            )
        send_share(step)
        return carry

    def one_share(step, carry):
        for head, rows, columns, own, row in owned_blocks(step):
            rounded, total = block_weights(
                q_ref[rows, columns], own, row, index_ref, bias_ref, kt_buf, causal, listed, factor
            )
            staged[head, rows, :] = block_mix(
                rounded[0],
                lambda n: jnp.concatenate([rounded[1 + n], rounded[2 + n]], axis=1),
                total,
                own, row, index_ref, v_buf, listed,
            )
        send_share(step)
        return carry

    lax.fori_loop(0, early * groups, weigh_early, 0)
    wait_cross(1)
    lax.fori_loop(0, early * groups, mix_early, 0)
    lax.fori_loop(early * groups, heads * groups, one_share, 0)

    for kv in range(2):
        for t in range(chain_len):
            for c in range(PIECES):
                if t < chain_len - 1:

                    @pl.when((place >= t) & has_next)
                    def _():
                        chain(t, kv, c).wait_send()

                @pl.when(sends_cross(t))
                def _():
                    cross(t, kv, c, side).wait_send()

    def finish(head, carry):
        out_own(head).wait()
        for r in range(groups - 1):
            out_copy(head, r).wait_send()
            out_in(head, r).wait_recv()
        return carry

    lax.fori_loop(0, heads, finish, 0)


def shards(queries, keys, values, vertical, slash):
    width = keys.shape[1]
    rows = queries.shape[0]
    blocks = rows // BLK
    heads = vertical.shape[0]
    slabs, groups = lax.axis_size("seq"), lax.axis_size("head")
    kt = jnp.swapaxes(keys.reshape(blocks, BLK, width), 1, 2)
    v = values.reshape(blocks, BLK, width)
    listed = slash.shape[1] + vertical.shape[1]
    early = min(EARLY, heads)
    dma = pltpu.SemaphoreType.DMA
    hops = (slabs // 2, 2, PIECES)
    smem, anywhere = pl.BlockSpec(memory_space=pltpu.SMEM), pl.BlockSpec(memory_space=pl.ANY)
    return pl.pallas_call(
        functools.partial(
            layer_kernel,
            blocks=blocks,
            listed=listed,
            width=width,
            heads=heads,
            slabs=slabs,
            groups=groups,
        ),
        in_specs=[smem, smem, anywhere, anywhere, anywhere],
        out_specs=anywhere,
        out_shape=jax.ShapeDtypeStruct((rows // groups, groups * heads * width), jnp.bfloat16),
        scratch_shapes=[
            pltpu.SMEM((heads * blocks * listed,), jnp.int32),
            pltpu.SMEM((heads * blocks * listed,), jnp.float32),
            pltpu.VMEM(queries.shape, jnp.bfloat16),
            pltpu.VMEM((slabs * blocks, width, BLK), jnp.bfloat16),
            pltpu.VMEM((slabs * blocks, BLK, width), jnp.bfloat16),
            pltpu.VMEM((heads, rows, width), jnp.bfloat16),
            pltpu.VMEM((early, rows, (listed + 1) * BLK), jnp.bfloat16),
            pltpu.VMEM((early, rows, width), jnp.float32),
            dma((3,)),
            dma(hops),
            dma(hops),
            dma(hops),
            dma(hops),
            dma((heads,)),
            dma((heads, groups - 1)),
            dma((heads, groups - 1)),
        ],
        compiler_params=pltpu.CompilerParams(
            collective_id=0, has_side_effects=True, vmem_limit_bytes=62 * 1024 * 1024
        ),
    )(slash, vertical, queries, kt, v)


def solution(mesh):
    in_specs = (
        P("seq", "head"),
        P("seq", "head"),
        P("seq", "head"),
        P("head", None),
        P("head", None),
    )
    out_specs = P(("seq", "head"), None)
    return jax.shard_map(shards, mesh=mesh, in_specs=in_specs, out_specs=out_specs, check_vma=False)
```

```python
import functools
import math

import jax
import jax.numpy as jnp
from jax import lax
from jax.experimental import pallas as pl
from jax.experimental.pallas import tpu as pltpu
from jax.sharding import PartitionSpec as P

BLK = 128
LARGEST_OFFSET = 28
CAP = 4
NEG = -1e30
PIECES = 2
EARLY = 6
VALUE_STRIDE = 3
MESH = pl.DeviceIdType.MESH


def block_weights(q, own, row, index_ref, bias_ref, kt_ref, causal, listed, factor):
    scores = [jnp.where(causal, jnp.dot(q, kt_ref[own], preferred_element_type=jnp.float32), NEG)]
    for n in range(0, listed, 2):
        a, b = index_ref[row + n], index_ref[row + n + 1]
        pair = jnp.dot(
            q, jnp.concatenate([kt_ref[a], kt_ref[b]], axis=1), preferred_element_type=jnp.float32
        )
        scores.append(pair[:, :BLK] + bias_ref[row + n])
        scores.append(pair[:, BLK:] + bias_ref[row + n + 1])
    top = functools.reduce(jnp.maximum, scores)
    top = jnp.max(top, axis=1, keepdims=True) * factor
    total = None
    rounded = []
    for s in scores:
        w = jnp.exp2(s * factor - top)
        total = w if total is None else total + w
        rounded.append(w.astype(jnp.bfloat16))
    return rounded, jnp.sum(total, axis=1, keepdims=True)


def block_mix(own_weights, pair_weights, total, own, row, index_ref, v_ref, listed):
    mixed = jnp.dot(own_weights, v_ref[own], preferred_element_type=jnp.float32)
    for n in range(0, listed, 2):
        a, b = index_ref[row + n], index_ref[row + n + 1]
        mixed += jnp.dot(
            pair_weights(n),
            jnp.concatenate([v_ref[a], v_ref[b]], axis=0),
            preferred_element_type=jnp.float32,
        )
    return (mixed / total).astype(jnp.bfloat16)


def layer_kernel(
    slash_ref,
    vertical_ref,
    queries_ref,
    kt_ref,
    v_ref,
    out_ref,
    index_ref,
    bias_ref,
    rank_ref,
    used_ref,
    found_ref,
    pack_ref,
    q_ref,
    kt_buf,
    v_buf,
    staged,
    early_weights,
    early_total,
    held,
    packed,
    held_sem,
    load_sem,
    chain_send,
    chain_recv,
    cross_send,
    cross_recv,
    out_local,
    out_send,
    out_recv,
    *,
    blocks,
    listed,
    width,
    heads,
    slabs,
    groups,
):
    slab = lax.axis_index("seq")
    group = lax.axis_index("head")
    chain_len = slabs // 2
    place, side = slab // 2, slab % 2
    piece = blocks // PIECES
    bufs = (kt_buf, v_buf)
    has_next = place + 1 < chain_len

    whole_blocks = slabs * blocks
    reach = (LARGEST_OFFSET + blocks - 1) // blocks
    pack_at = reach // 2
    cap_piece = CAP // PIECES

    def part(kv, place_of, side_of, c, far):
        origin = place_of * 2 + side_of
        if far:
            first = pl.multiple_of(whole_blocks + origin * CAP + c * cap_piece, cap_piece)
            return bufs[kv].at[pl.ds(first, cap_piece)]
        first = pl.multiple_of(origin * blocks + c * piece, piece)
        return bufs[kv].at[pl.ds(first, piece)]

    def sent(ref, t, kv, c, far):
        if t == pack_at and far:
            return packed.at[kv, pl.ds(c * cap_piece, cap_piece)]
        return ref

    def chain(t, kv, c):
        ref = part(kv, place - t, side, c, chain_far(t + 1))
        return pltpu.make_async_remote_copy(
            sent(ref, t, kv, c, chain_far(t + 1)), ref, chain_send.at[t, kv, c], chain_recv.at[t, kv, c],
            device_id={"seq": slab + 2}, device_id_type=MESH,
        )

    def chain_in(t, kv, c):
        ref = part(kv, place - t, side, c, chain_far(t))
        return pltpu.make_async_remote_copy(
            ref, ref, chain_send.at[t - 1, kv, c], chain_recv.at[t - 1, kv, c],
            device_id={"seq": slab - 2}, device_id_type=MESH,
        )

    def cross(t, kv, c, sender):
        ref = part(kv, place - t, sender, c, cross_far(t, sender))
        return pltpu.make_async_remote_copy(
            sent(ref, t, kv, c, cross_far(t, sender)), ref, cross_send.at[t, kv, c], cross_recv.at[t, kv, c],
            device_id={"seq": place * 2 + 1 - side}, device_id_type=MESH,
        )

    def chain_far(t):
        return 2 * t > reach

    def cross_far(t, sender):
        return (2 * t - 1 if sender else 2 * t + 1) > reach

    def cross_runs(t, sender, this_side):
        if t == 0 and sender == 1:
            return None
        return (side == this_side) & (place >= t)

    own_first = pl.multiple_of(slab * blocks, blocks)
    loads = [
        pltpu.make_async_copy(src, buf.at[pl.ds(own_first, blocks)], load_sem.at[kv])
        for kv, (src, buf) in enumerate(((kt_ref, kt_buf), (v_ref, v_buf)))
    ]
    loads.append(pltpu.make_async_copy(queries_ref, q_ref, load_sem.at[2]))
    for load in loads:
        load.start()

    barrier = pltpu.get_barrier_semaphore()
    pl.semaphore_signal(
        barrier, 1, device_id={"seq": place * 2 + 1 - side}, device_id_type=MESH
    )
    for d in range(1, groups):
        pl.semaphore_signal(
            barrier, 1, device_id={"head": lax.rem(group + d, groups)}, device_id_type=MESH
        )

    @pl.when(has_next)
    def _():
        pl.semaphore_signal(barrier, 1, device_id={"seq": slab + 2}, device_id_type=MESH)

    @pl.when(place > 0)
    def _():
        pl.semaphore_signal(barrier, 1, device_id={"seq": slab - 2}, device_id_type=MESH)

    pl.semaphore_wait(
        barrier, groups + has_next.astype(jnp.int32) + (place > 0).astype(jnp.int32)
    )
    def start_cross(t, kv, c, packed):
        for sender in range(2):
            runs = cross_runs(t, sender, sender)
            if runs is not None and (t == pack_at and cross_far(t, sender)) == packed:

                @pl.when(runs)
                def _():
                    cross(t, kv, c, sender).start()

    def start_chain(t, kv, c, packed):
        if t < chain_len - 1 and (t == pack_at and chain_far(t + 1)) == packed:

            @pl.when((place >= t) & has_next)
            def _():
                chain(t, kv, c).start()

    def pass_on(t, kv, c):
        if t > 0:

            @pl.when(place >= t)
            def _():
                chain_in(t, kv, c).wait_recv()

        start_chain(t, kv, c, False)
        start_cross(t, kv, c, False)
        if t == pack_at and c == PIECES - 1:

            @pl.when(place >= t)
            def _():
                first = pl.multiple_of(((place - t) * 2 + side) * blocks, blocks)
                move = pltpu.make_async_copy(
                    bufs[kv].at[pl.ds(first, blocks)], held.at[kv], held_sem.at[kv]
                )
                move.start()
                move.wait()
                for k in range(CAP):
                    picked = held[kv, 0].astype(jnp.float32) * pack_ref[k * blocks]
                    for n in range(1, blocks):
                        picked += held[kv, n].astype(jnp.float32) * pack_ref[k * blocks + n]
                    packed[kv, k] = picked.astype(jnp.bfloat16)

            for each in range(PIECES):
                start_chain(t, kv, each, True)
                start_cross(t, kv, each, True)

    def wait_cross(kv):
        for t in range(chain_len):
            for c in range(PIECES):
                for sender in range(2):
                    runs = cross_runs(t, sender, 1 - sender)
                    if runs is not None:

                        @pl.when(runs)
                        def _():
                            cross(t, kv, c, sender).wait_recv()

    base = slab * blocks
    slashes, verticals = slash_ref.shape[1], vertical_ref.shape[1]

    def rank_block(block, rank):
        used = block < 0
        for head in range(heads):
            for n in range(verticals):
                used = used | (vertical_ref[head, n] == block)
        rank = jnp.where(block % blocks == 0, 0, rank)
        rank_ref[block] = rank
        used_ref[block] = used.astype(jnp.int32)
        return rank + used.astype(jnp.int32)

    def place_verticals(head, carry):
        for n in range(verticals):
            block = vertical_ref[head, n]
            far = whole_blocks + (block // blocks) * CAP + rank_ref[block]
            found_ref[head * verticals + n] = jnp.where(
                block >= (slab - reach) * blocks, block, far
            )
        return carry

    def list_blocks(step, carry):
        head, own = step // blocks, base + step % blocks
        reached = [own - slash_ref[head, n] for n in range(slashes)]
        for n, block in enumerate(reached):
            ok = block >= 0
            index_ref[step * listed + n] = jnp.where(ok, block, own)
            bias_ref[step * listed + n] = jnp.where(ok, 0.0, NEG)
        for n in range(verticals):
            block = vertical_ref[head, n]
            ok = block < own
            for other in reached:
                ok = ok & (block != other)
            found = found_ref[head * verticals + n]
            index_ref[step * listed + slashes + n] = jnp.where(ok, found, own)
            bias_ref[step * listed + slashes + n] = jnp.where(ok, 0.0, NEG)
        return carry

    lists = heads * blocks
    loads[0].wait()
    for c in range(PIECES):
        pass_on(0, 0, c)
    lax.fori_loop(0, whole_blocks, rank_block, jnp.int32(0))
    packed_first = jnp.maximum((place - pack_at) * 2 + side, 0) * blocks
    for k in range(CAP):
        for n in range(blocks):
            block = packed_first + n
            hit = (used_ref[block] == 1) & (rank_ref[block] == k)
            pack_ref[k * blocks + n] = jnp.where(hit, 1.0, 0.0)
    for t in range(1, chain_len):
        for c in range(PIECES):
            pass_on(t, 0, c)
        if t == 1:
            lax.fori_loop(0, heads, place_verticals, 0)
            lax.fori_loop(0, lists // 4, list_blocks, 0)
        if t == 2:
            lax.fori_loop(lists // 4, lists // 2, list_blocks, 0)
    loads[1].wait()
    for c in range(PIECES):
        pass_on(0, 1, c)
    lax.fori_loop(lists // 2, lists, list_blocks, 0)
    wait_cross(0)
    loads[2].wait()

    factor = math.log2(math.e) / math.sqrt(width)
    causal = lax.broadcasted_iota(jnp.int32, (BLK, BLK), 0) >= lax.broadcasted_iota(
        jnp.int32, (BLK, BLK), 1
    )
    share = blocks // groups
    share_rows = share * BLK

    def out_columns(group_of, head):
        return pl.ds(pl.multiple_of((group_of * heads + head) * width, width), width)

    def out_copy(head, r):
        owner = lax.rem(group + 1 + r, groups)
        return pltpu.make_async_remote_copy(
            staged.at[head, pl.ds(pl.multiple_of(owner * share_rows, share_rows), share_rows)],
            out_ref.at[:, out_columns(group, head)],
            out_send.at[head, r], out_recv.at[head, r],
            device_id={"head": owner}, device_id_type=MESH,
        )

    def out_in(head, r):
        sender = lax.rem(group + groups - 1 - r, groups)
        return pltpu.make_async_remote_copy(
            staged.at[head, pl.ds(0, share_rows)],
            out_ref.at[:, out_columns(sender, head)],
            out_send.at[head, r], out_recv.at[head, r],
            device_id={"head": sender}, device_id_type=MESH,
        )

    def out_own(head):
        return pltpu.make_async_copy(
            staged.at[head, pl.ds(pl.multiple_of(group * share_rows, share_rows), share_rows)],
            out_ref.at[:, out_columns(group, head)],
            out_local.at[head],
        )

    early = early_weights.shape[0]
    values_due = []
    for t in range(1, chain_len):
        each = [[(t, c)] for c in range(PIECES)]
        values_due += [sum(each, [])] if t == pack_at else each

    def owned_blocks(step):
        head, r = step // groups, step % groups
        owner = lax.rem(group + 1 + r, groups)
        columns = pl.ds(pl.multiple_of(head * width, width), width)
        for u in range(share):
            i = owner * share + u
            rows = pl.ds(pl.multiple_of(i * BLK, BLK), BLK)
            yield head, rows, columns, base + i, (head * blocks + i) * listed

    def send_share(step):
        head, r = step // groups, step % groups

        @pl.when(r < groups - 1)
        def _():
            out_copy(head, r).start()

        @pl.when(r == groups - 1)
        def _():
            out_own(head).start()

    def weigh_early(step, carry):
        for k, due in enumerate(values_due):

            @pl.when(step == min(VALUE_STRIDE * (k + 1), early * groups - 1))
            def _():
                for t, c in due:
                    pass_on(t, 1, c)

        for head, rows, columns, own, row in owned_blocks(step):
            rounded, total = block_weights(
                q_ref[rows, columns], own, row, index_ref, bias_ref, kt_buf, causal, listed, factor
            )
            for n, w in enumerate(rounded):
                early_weights[head, rows, n * BLK : (n + 1) * BLK] = w
            early_total[head, rows, :] = jnp.broadcast_to(total, (BLK, width))
        return carry

    def mix_early(step, carry):
        for head, rows, columns, own, row in owned_blocks(step):
            staged[head, rows, :] = block_mix(
                early_weights[head, rows, :BLK],
                lambda n: early_weights[head, rows, (n + 1) * BLK : (n + 3) * BLK],
                early_total[head, rows, :],
                own, row, index_ref, v_buf, listed,
            )
        send_share(step)
        return carry

    def one_share(step, carry):
        for head, rows, columns, own, row in owned_blocks(step):
            rounded, total = block_weights(
                q_ref[rows, columns], own, row, index_ref, bias_ref, kt_buf, causal, listed, factor
            )
            staged[head, rows, :] = block_mix(
                rounded[0],
                lambda n: jnp.concatenate([rounded[1 + n], rounded[2 + n]], axis=1),
                total,
                own, row, index_ref, v_buf, listed,
            )
        send_share(step)
        return carry

    lax.fori_loop(0, early * groups, weigh_early, 0)
    wait_cross(1)
    lax.fori_loop(0, early * groups, mix_early, 0)
    lax.fori_loop(early * groups, heads * groups, one_share, 0)

    for kv in range(2):
        for t in range(chain_len):
            for c in range(PIECES):
                if t < chain_len - 1:

                    @pl.when((place >= t) & has_next)
                    def _():
                        chain(t, kv, c).wait_send()

                for sender in range(2):
                    runs = cross_runs(t, sender, sender)
                    if runs is not None:

                        @pl.when(runs)
                        def _():
                            cross(t, kv, c, sender).wait_send()

    def finish(head, carry):
        out_own(head).wait()
        for r in range(groups - 1):
            out_copy(head, r).wait_send()
            out_in(head, r).wait_recv()
        return carry

    lax.fori_loop(0, heads, finish, 0)


def shards(queries, keys, values, vertical, slash):
    width = keys.shape[1]
    rows = queries.shape[0]
    blocks = rows // BLK
    heads = vertical.shape[0]
    slabs, groups = lax.axis_size("seq"), lax.axis_size("head")
    kt = jnp.swapaxes(keys.reshape(blocks, BLK, width), 1, 2)
    v = values.reshape(blocks, BLK, width)
    listed = slash.shape[1] + vertical.shape[1]
    early = min(EARLY, heads)
    dma = pltpu.SemaphoreType.DMA
    hops = (slabs // 2, 2, PIECES)
    smem, anywhere = pl.BlockSpec(memory_space=pltpu.SMEM), pl.BlockSpec(memory_space=pl.ANY)
    return pl.pallas_call(
        functools.partial(
            layer_kernel,
            blocks=blocks,
            listed=listed,
            width=width,
            heads=heads,
            slabs=slabs,
            groups=groups,
        ),
        in_specs=[smem, smem, anywhere, anywhere, anywhere],
        out_specs=anywhere,
        out_shape=jax.ShapeDtypeStruct((rows // groups, groups * heads * width), jnp.bfloat16),
        scratch_shapes=[
            pltpu.SMEM((heads * blocks * listed,), jnp.int32),
            pltpu.SMEM((heads * blocks * listed,), jnp.float32),
            pltpu.SMEM((slabs * blocks,), jnp.int32),
            pltpu.SMEM((slabs * blocks,), jnp.int32),
            pltpu.SMEM((vertical.size,), jnp.int32),
            pltpu.SMEM((CAP * blocks,), jnp.float32),
            pltpu.VMEM(queries.shape, jnp.bfloat16),
            pltpu.VMEM((slabs * (blocks + CAP), width, BLK), jnp.bfloat16),
            pltpu.VMEM((slabs * (blocks + CAP), BLK, width), jnp.bfloat16),
            pltpu.VMEM((heads, rows, width), jnp.bfloat16),
            pltpu.VMEM((early, rows, (listed + 1) * BLK), jnp.bfloat16),
            pltpu.VMEM((early, rows, width), jnp.float32),
            pltpu.VMEM((2, blocks, BLK, width), jnp.bfloat16),
            pltpu.VMEM((2, CAP, BLK, width), jnp.bfloat16),
            dma((2,)),
            dma((3,)),
            dma(hops),
            dma(hops),
            dma(hops),
            dma(hops),
            dma((heads,)),
            dma((heads, groups - 1)),
            dma((heads, groups - 1)),
        ],
        compiler_params=pltpu.CompilerParams(
            collective_id=0, has_side_effects=True, vmem_limit_bytes=62 * 1024 * 1024
        ),
    )(slash, vertical, queries, kt, v)


def solution(mesh):
    in_specs = (
        P("seq", "head"),
        P("seq", "head"),
        P("seq", "head"),
        P("head", None),
        P("head", None),
    )
    out_specs = P(("seq", "head"), None)
    return jax.shard_map(shards, mesh=mesh, in_specs=in_specs, out_specs=out_specs, check_vma=False)
```

```python
import functools
import math

import jax
import jax.numpy as jnp
from jax import lax
from jax.experimental import pallas as pl
from jax.experimental.pallas import tpu as pltpu
from jax.sharding import PartitionSpec as P

BLK = 128
LARGEST_OFFSET = 28
CAP = 4
NEG = -1e30
PIECES = 2
EARLY = 6
VALUE_STRIDE = 3
MESH = pl.DeviceIdType.MESH


def block_weights(q, own, row, index_ref, bias_ref, kt_ref, causal, listed, factor):
    scores = [jnp.where(causal, jnp.dot(q, kt_ref[own], preferred_element_type=jnp.float32), NEG)]
    for n in range(0, listed, 2):
        a, b = index_ref[row + n], index_ref[row + n + 1]
        pair = jnp.dot(
            q, jnp.concatenate([kt_ref[a], kt_ref[b]], axis=1), preferred_element_type=jnp.float32
        )
        scores.append(pair[:, :BLK] + bias_ref[row + n])
        scores.append(pair[:, BLK:] + bias_ref[row + n + 1])
    top = functools.reduce(jnp.maximum, scores)
    top = jnp.max(top, axis=1, keepdims=True) * factor
    total = None
    rounded = []
    for s in scores:
        w = jnp.exp2(s * factor - top)
        total = w if total is None else total + w
        rounded.append(w.astype(jnp.bfloat16))
    return rounded, jnp.sum(total, axis=1, keepdims=True)


def block_mix(own_weights, pair_weights, total, own, row, index_ref, v_ref, listed):
    mixed = jnp.dot(own_weights, v_ref[own], preferred_element_type=jnp.float32)
    for n in range(0, listed, 2):
        a, b = index_ref[row + n], index_ref[row + n + 1]
        mixed += jnp.dot(
            pair_weights(n),
            jnp.concatenate([v_ref[a], v_ref[b]], axis=0),
            preferred_element_type=jnp.float32,
        )
    return (mixed / total).astype(jnp.bfloat16)


def layer_kernel(
    slash_ref,
    vertical_ref,
    queries_ref,
    kt_ref,
    v_ref,
    out_ref,
    index_ref,
    bias_ref,
    rank_ref,
    used_ref,
    found_ref,
    pack_ref,
    q_ref,
    kt_buf,
    v_buf,
    staged,
    early_weights,
    early_total,
    held,
    packed,
    held_sem,
    load_sem,
    chain_send,
    chain_recv,
    cross_send,
    cross_recv,
    out_local,
    out_send,
    out_recv,
    *,
    blocks,
    listed,
    width,
    heads,
    slabs,
    groups,
):
    slab = lax.axis_index("seq")
    group = lax.axis_index("head")
    chain_len = slabs // 2
    place, side = slab // 2, slab % 2
    piece = blocks // PIECES
    bufs = (kt_buf, v_buf)
    has_next = place + 1 < chain_len

    whole_blocks = slabs * blocks
    reach = (LARGEST_OFFSET + blocks - 1) // blocks
    pack_at = reach // 2
    cap_piece = CAP // PIECES

    def part(kv, place_of, side_of, c, far):
        origin = place_of * 2 + side_of
        if far:
            first = pl.multiple_of(whole_blocks + origin * CAP + c * cap_piece, cap_piece)
            return bufs[kv].at[pl.ds(first, cap_piece)]
        first = pl.multiple_of(origin * blocks + c * piece, piece)
        return bufs[kv].at[pl.ds(first, piece)]

    def sent(ref, t, kv, c, far):
        if t == pack_at and far:
            return packed.at[kv, pl.ds(c * cap_piece, cap_piece)]
        return ref

    def chain(t, kv, c):
        ref = part(kv, place - t, side, c, chain_far(t + 1))
        return pltpu.make_async_remote_copy(
            sent(ref, t, kv, c, chain_far(t + 1)), ref, chain_send.at[t, kv, c], chain_recv.at[t, kv, c],
            device_id={"seq": slab + 2}, device_id_type=MESH,
        )

    def chain_in(t, kv, c):
        ref = part(kv, place - t, side, c, chain_far(t))
        return pltpu.make_async_remote_copy(
            ref, ref, chain_send.at[t - 1, kv, c], chain_recv.at[t - 1, kv, c],
            device_id={"seq": slab - 2}, device_id_type=MESH,
        )

    def cross(t, kv, c, sender):
        ref = part(kv, place - t, sender, c, cross_far(t, sender))
        return pltpu.make_async_remote_copy(
            sent(ref, t, kv, c, cross_far(t, sender)), ref, cross_send.at[t, kv, c], cross_recv.at[t, kv, c],
            device_id={"seq": place * 2 + 1 - side}, device_id_type=MESH,
        )

    def chain_far(t):
        return 2 * t > reach

    def cross_far(t, sender):
        return (2 * t - 1 if sender else 2 * t + 1) > reach

    def cross_runs(t, sender, this_side):
        if t == 0 and sender == 1:
            return None
        return (side == this_side) & (place >= t)

    own_first = pl.multiple_of(slab * blocks, blocks)
    loads = [
        pltpu.make_async_copy(src, buf.at[pl.ds(own_first, blocks)], load_sem.at[kv])
        for kv, (src, buf) in enumerate(((kt_ref, kt_buf), (v_ref, v_buf)))
    ]
    loads.append(pltpu.make_async_copy(queries_ref, q_ref, load_sem.at[2]))
    for load in loads:
        load.start()

    barrier = pltpu.get_barrier_semaphore()
    pl.semaphore_signal(
        barrier, 1, device_id={"seq": place * 2 + 1 - side}, device_id_type=MESH
    )
    for d in range(1, groups):
        pl.semaphore_signal(
            barrier, 1, device_id={"head": lax.rem(group + d, groups)}, device_id_type=MESH
        )

    @pl.when(has_next)
    def _():
        pl.semaphore_signal(barrier, 1, device_id={"seq": slab + 2}, device_id_type=MESH)

    @pl.when(place > 0)
    def _():
        pl.semaphore_signal(barrier, 1, device_id={"seq": slab - 2}, device_id_type=MESH)

    pl.semaphore_wait(
        barrier, groups + has_next.astype(jnp.int32) + (place > 0).astype(jnp.int32)
    )
    def start_cross(t, kv, c, packed):
        for sender in range(2):
            runs = cross_runs(t, sender, sender)
            if runs is not None and (t == pack_at and cross_far(t, sender)) == packed:

                @pl.when(runs)
                def _():
                    cross(t, kv, c, sender).start()

    def start_chain(t, kv, c, packed):
        if t < chain_len - 1 and (t == pack_at and chain_far(t + 1)) == packed:

            @pl.when((place >= t) & has_next)
            def _():
                chain(t, kv, c).start()

    def pass_on(t, kv, c):
        if t > 0:

            @pl.when(place >= t)
            def _():
                chain_in(t, kv, c).wait_recv()

        start_chain(t, kv, c, False)
        start_cross(t, kv, c, False)
        if t == pack_at and c == PIECES - 1:

            @pl.when(place >= t)
            def _():
                first = pl.multiple_of(((place - t) * 2 + side) * blocks, blocks)
                move = pltpu.make_async_copy(
                    bufs[kv].at[pl.ds(first, blocks)], held.at[kv], held_sem.at[kv]
                )
                move.start()
                move.wait()
                for k in range(CAP):
                    picked = held[kv, 0].astype(jnp.float32) * pack_ref[k * blocks]
                    for n in range(1, blocks):
                        picked += held[kv, n].astype(jnp.float32) * pack_ref[k * blocks + n]
                    packed[kv, k] = picked.astype(jnp.bfloat16)

            for each in range(PIECES):
                start_chain(t, kv, each, True)
                start_cross(t, kv, each, True)

    def wait_cross(kv):
        for t in range(chain_len):
            for c in range(PIECES):
                for sender in range(2):
                    runs = cross_runs(t, sender, 1 - sender)
                    if runs is not None:

                        @pl.when(runs)
                        def _():
                            cross(t, kv, c, sender).wait_recv()

    base = slab * blocks
    slashes, verticals = slash_ref.shape[1], vertical_ref.shape[1]

    def rank_block(block, rank):
        used = block < 0
        for head in range(heads):
            for n in range(verticals):
                used = used | (vertical_ref[head, n] == block)
        rank = jnp.where(block % blocks == 0, 0, rank)
        rank_ref[block] = rank
        used_ref[block] = used.astype(jnp.int32)
        return rank + used.astype(jnp.int32)

    def place_verticals(head, carry):
        for n in range(verticals):
            block = vertical_ref[head, n]
            far = whole_blocks + (block // blocks) * CAP + rank_ref[block]
            found_ref[head * verticals + n] = jnp.where(
                block >= (slab - reach) * blocks, block, far
            )
        return carry

    def list_block(head, own, row):
        reached = [own - slash_ref[head, n] for n in range(slashes)]
        for n, block in enumerate(reached):
            ok = block >= 0
            index_ref[row + n] = jnp.where(ok, block, own)
            bias_ref[row + n] = jnp.where(ok, 0.0, NEG)
        for n in range(verticals):
            block = vertical_ref[head, n]
            ok = block < own
            for other in reached:
                ok = ok & (block != other)
            found = found_ref[head * verticals + n]
            index_ref[row + slashes + n] = jnp.where(ok, found, own)
            bias_ref[row + slashes + n] = jnp.where(ok, 0.0, NEG)

    loads[0].wait()
    for c in range(PIECES):
        pass_on(0, 0, c)
    lax.fori_loop(0, whole_blocks, rank_block, jnp.int32(0))
    packed_first = jnp.maximum((place - pack_at) * 2 + side, 0) * blocks
    for k in range(CAP):
        for n in range(blocks):
            block = packed_first + n
            hit = (used_ref[block] == 1) & (rank_ref[block] == k)
            pack_ref[k * blocks + n] = jnp.where(hit, 1.0, 0.0)
    for t in range(1, chain_len):
        for c in range(PIECES):
            pass_on(t, 0, c)
        if t == 1:
            lax.fori_loop(0, heads, place_verticals, 0)
    loads[1].wait()
    for c in range(PIECES):
        pass_on(0, 1, c)
    loads[2].wait()

    factor = math.log2(math.e) / math.sqrt(width)
    causal = lax.broadcasted_iota(jnp.int32, (BLK, BLK), 0) >= lax.broadcasted_iota(
        jnp.int32, (BLK, BLK), 1
    )
    share = blocks // groups
    share_rows = share * BLK

    def out_columns(group_of, head):
        return pl.ds(pl.multiple_of((group_of * heads + head) * width, width), width)

    def out_copy(head, r):
        owner = lax.rem(group + 1 + r, groups)
        return pltpu.make_async_remote_copy(
            staged.at[head, pl.ds(pl.multiple_of(owner * share_rows, share_rows), share_rows)],
            out_ref.at[:, out_columns(group, head)],
            out_send.at[head, r], out_recv.at[head, r],
            device_id={"head": owner}, device_id_type=MESH,
        )

    def out_in(head, r):
        sender = lax.rem(group + groups - 1 - r, groups)
        return pltpu.make_async_remote_copy(
            staged.at[head, pl.ds(0, share_rows)],
            out_ref.at[:, out_columns(sender, head)],
            out_send.at[head, r], out_recv.at[head, r],
            device_id={"head": sender}, device_id_type=MESH,
        )

    def out_own(head):
        return pltpu.make_async_copy(
            staged.at[head, pl.ds(pl.multiple_of(group * share_rows, share_rows), share_rows)],
            out_ref.at[:, out_columns(group, head)],
            out_local.at[head],
        )

    early = early_weights.shape[0]
    values_due = []
    for t in range(1, chain_len):
        each = [[(t, c)] for c in range(PIECES)]
        values_due += [sum(each, [])] if t == pack_at else each

    def owned_blocks(step):
        head, r = step // groups, step % groups
        owner = lax.rem(group + 1 + r, groups)
        columns = pl.ds(pl.multiple_of(head * width, width), width)
        for u in range(share):
            i = owner * share + u
            rows = pl.ds(pl.multiple_of(i * BLK, BLK), BLK)
            yield head, rows, columns, base + i, (head * blocks + i) * listed

    def list_share(step):
        for head, rows, columns, own, row in owned_blocks(step):
            list_block(head, own, row)

    def list_next(step):
        list_share(jnp.minimum(step + 1, heads * groups - 1))

    def send_share(step):
        head, r = step // groups, step % groups

        @pl.when(r < groups - 1)
        def _():
            out_copy(head, r).start()

        @pl.when(r == groups - 1)
        def _():
            out_own(head).start()

    def weigh_early(step, carry):
        for k, due in enumerate(values_due):

            @pl.when(step == min(VALUE_STRIDE * (k + 1), early * groups - 1))
            def _():
                for t, c in due:
                    pass_on(t, 1, c)

        list_next(step)
        for head, rows, columns, own, row in owned_blocks(step):
            rounded, total = block_weights(
                q_ref[rows, columns], own, row, index_ref, bias_ref, kt_buf, causal, listed, factor
            )
            for n, w in enumerate(rounded):
                early_weights[head, rows, n * BLK : (n + 1) * BLK] = w
            early_total[head, rows, :] = jnp.broadcast_to(total, (BLK, width))
        return carry

    def mix_early(step, carry):
        for head, rows, columns, own, row in owned_blocks(step):
            staged[head, rows, :] = block_mix(
                early_weights[head, rows, :BLK],
                lambda n: early_weights[head, rows, (n + 1) * BLK : (n + 3) * BLK],
                early_total[head, rows, :],
                own, row, index_ref, v_buf, listed,
            )
        send_share(step)
        return carry

    def one_share(step, carry):
        list_next(step)
        for head, rows, columns, own, row in owned_blocks(step):
            rounded, total = block_weights(
                q_ref[rows, columns], own, row, index_ref, bias_ref, kt_buf, causal, listed, factor
            )
            staged[head, rows, :] = block_mix(
                rounded[0],
                lambda n: jnp.concatenate([rounded[1 + n], rounded[2 + n]], axis=1),
                total,
                own, row, index_ref, v_buf, listed,
            )
        send_share(step)
        return carry

    list_share(jnp.int32(0))
    wait_cross(0)
    lax.fori_loop(0, early * groups, weigh_early, 0)
    wait_cross(1)
    lax.fori_loop(0, early * groups, mix_early, 0)
    lax.fori_loop(early * groups, heads * groups, one_share, 0)

    for kv in range(2):
        for t in range(chain_len):
            for c in range(PIECES):
                if t < chain_len - 1:

                    @pl.when((place >= t) & has_next)
                    def _():
                        chain(t, kv, c).wait_send()

                for sender in range(2):
                    runs = cross_runs(t, sender, sender)
                    if runs is not None:

                        @pl.when(runs)
                        def _():
                            cross(t, kv, c, sender).wait_send()

    def finish(head, carry):
        out_own(head).wait()
        for r in range(groups - 1):
            out_copy(head, r).wait_send()
            out_in(head, r).wait_recv()
        return carry

    lax.fori_loop(0, heads, finish, 0)


def shards(queries, keys, values, vertical, slash):
    width = keys.shape[1]
    rows = queries.shape[0]
    blocks = rows // BLK
    heads = vertical.shape[0]
    slabs, groups = lax.axis_size("seq"), lax.axis_size("head")
    kt = jnp.swapaxes(keys.reshape(blocks, BLK, width), 1, 2)
    v = values.reshape(blocks, BLK, width)
    listed = slash.shape[1] + vertical.shape[1]
    early = min(EARLY, heads)
    dma = pltpu.SemaphoreType.DMA
    hops = (slabs // 2, 2, PIECES)
    smem, anywhere = pl.BlockSpec(memory_space=pltpu.SMEM), pl.BlockSpec(memory_space=pl.ANY)
    return pl.pallas_call(
        functools.partial(
            layer_kernel,
            blocks=blocks,
            listed=listed,
            width=width,
            heads=heads,
            slabs=slabs,
            groups=groups,
        ),
        in_specs=[smem, smem, anywhere, anywhere, anywhere],
        out_specs=anywhere,
        out_shape=jax.ShapeDtypeStruct((rows // groups, groups * heads * width), jnp.bfloat16),
        scratch_shapes=[
            pltpu.SMEM((heads * blocks * listed,), jnp.int32),
            pltpu.SMEM((heads * blocks * listed,), jnp.float32),
            pltpu.SMEM((slabs * blocks,), jnp.int32),
            pltpu.SMEM((slabs * blocks,), jnp.int32),
            pltpu.SMEM((vertical.size,), jnp.int32),
            pltpu.SMEM((CAP * blocks,), jnp.float32),
            pltpu.VMEM(queries.shape, jnp.bfloat16),
            pltpu.VMEM((slabs * (blocks + CAP), width, BLK), jnp.bfloat16),
            pltpu.VMEM((slabs * (blocks + CAP), BLK, width), jnp.bfloat16),
            pltpu.VMEM((heads, rows, width), jnp.bfloat16),
            pltpu.VMEM((early, rows, (listed + 1) * BLK), jnp.bfloat16),
            pltpu.VMEM((early, rows, width), jnp.float32),
            pltpu.VMEM((2, blocks, BLK, width), jnp.bfloat16),
            pltpu.VMEM((2, CAP, BLK, width), jnp.bfloat16),
            dma((2,)),
            dma((3,)),
            dma(hops),
            dma(hops),
            dma(hops),
            dma(hops),
            dma((heads,)),
            dma((heads, groups - 1)),
            dma((heads, groups - 1)),
        ],
        compiler_params=pltpu.CompilerParams(
            collective_id=0, has_side_effects=True, vmem_limit_bytes=62 * 1024 * 1024
        ),
    )(slash, vertical, queries, kt, v)


def solution(mesh):
    in_specs = (
        P("seq", "head"),
        P("seq", "head"),
        P("seq", "head"),
        P("head", None),
        P("head", None),
    )
    out_specs = P(("seq", "head"), None)
    return jax.shard_map(shards, mesh=mesh, in_specs=in_specs, out_specs=out_specs, check_vma=False)
```
